32 devices in a mesh: expert: 8 (over z, core), shard: 4 (over y, x).
Axes of the slice: x: 2, y: 2, z: 4, core: 2. Of those that a mesh axis runs over, the one named last changes fastest.
Arguments:
- w_down: float32 [64, 1024, 2048], P('expert', None, 'shard'), may hold values from -0.25 to 0.25
- avg_down: float32 [64, 1024, 2048], P('expert', None, 'shard'), may hold values from -0.1875 to 0.1875
- mix_share: float32 [64], P('expert'), may hold values from 0.2 to 0.8
- router_weight: float32 [2048, 64], P('shard', 'expert'), may hold values from -0.125 to 0.125
- router_gain: float32 [2048], P('shard'), may hold values from 0.25 to 1.75
Outputs:
- serve_down: bfloat16 [64, 1024, 2048], P('expert')
- scale_down: float32 [64, 1024], P('expert')
- serve_router: bfloat16 [2048, 64], replicated
The draws below stay inside these ranges and needn't reach their ends.
All inputs are finite; a program needn't handle non-finite values. Where the reference program divides by a largest or mean magnitude, that divisor is 1e-20 or more.
Results may differ from the reference program's by a relative error of at most 0.001.
Values may be sent and summed in bfloat16 or wider, within the bound.
A program may use at most 192 MiB of HBM per device.

```python
import jax
import jax.numpy as jnp

EXPERTS = 64
D_MODEL = 2048
D_EXPERT = 1024


def strengthened(values, stream_key, source, target, blocks, factor):
    def block_of(dim):
        return (jnp.arange(values.shape[dim]) // (values.shape[dim] // blocks)).reshape((-1,) + (1,) * (values.ndim - 1 - dim))

    one_side = jax.random.permutation(stream_key, blocks)[block_of(target)]
    second = (block_of(target) + blocks // 2) % blocks
    return jnp.where((block_of(source) == one_side) | (block_of(source) == second), factor * values, values)


def block_levels(key, extent, pieces, low, largest):
    level, own = 1.0, jax.random.fold_in(key, 6)
    for position, blocks in pieces:
        steps = jnp.exp(jax.random.uniform(jax.random.fold_in(own, position), (blocks,), jnp.float32, low / len(pieces), largest / len(pieces)))
        level = level * jnp.repeat(steps, extent[position] // blocks).reshape([-1 if axis == position else 1 for axis in range(len(extent))])
    return level


def centred(key, dims, width, most, split=(), held_as=jnp.bfloat16):
    values = width * jax.random.normal(key, dims, jnp.float32)
    if split:
        values = values * block_levels(key, dims, split, -0.22, 0.18)
    return jnp.clip(values, -most, most).astype(held_as)


def gaussian_with(key, dims, width, bound, split, heavy, kind=jnp.bfloat16):
    result = width * jax.random.normal(key, dims, jnp.float32)
    if split:
        result = result * block_levels(key, dims, split, -0.22, 0.18)
    return jnp.clip(strengthened(result, jax.random.fold_in(key, 3), *heavy), -bound, bound).astype(kind)


def setup_inputs(seed: int = 0) -> dict:
    key_list = jax.random.split(jax.random.key(seed), 6)
    return {
        "w_down": gaussian_with(key_list[0], (EXPERTS, D_EXPERT, D_MODEL), D_EXPERT ** -0.5, 0.25, ((0, 8), (2, 4)), (2, 1, 4, 2.0), jnp.float32),
        "avg_down": centred(key_list[1], (EXPERTS, D_EXPERT, D_MODEL), D_EXPERT ** -0.5, 0.1875, ((0, 8), (2, 4)), jnp.float32),
        "mix_share": jnp.clip(0.2 + 0.6 * jax.random.uniform(key_list[2], (EXPERTS,), jnp.float32) ** block_levels(key_list[2], (EXPERTS,), ((0, 8),), -0.2, 0.2), 0.2, 0.8),
        "router_weight": centred(key_list[3], (D_MODEL, EXPERTS), D_MODEL ** -0.5, 0.125, ((0, 4), (1, 8)), jnp.float32),
        "router_gain": jnp.clip(1.0 + 0.15 * jax.random.normal(key_list[4], (D_MODEL,), jnp.float32), 0.25, 1.75),
    }


def reference(w_down, avg_down, mix_share, router_weight, router_gain):
    fresh_down = mix_share[:, None, None] * w_down + (1.0 - mix_share[:, None, None]) * avg_down
    scale_down = jnp.sum(jnp.abs(fresh_down), axis=2) / D_MODEL
    serve_down = (fresh_down / jnp.expand_dims(scale_down, 2)).astype(jnp.bfloat16)
    serve_router = (router_weight * router_gain[:, None]).astype(jnp.bfloat16)
    return serve_down, scale_down, serve_router
```

```python
import functools
import math

import jax
import jax.numpy as jnp
from jax import lax
from jax.experimental import pallas as pl
from jax.experimental.pallas import tpu as pltpu
from jax.sharding import PartitionSpec as P

MESH = pl.DeviceIdType.MESH
LANES = 128
LOADS = 3
LAG = 2


def gather_kernel(
    shards, groups, width,
    mix_ref, w_ref, avg_ref, rw_ref, rg_ref,
    out_ref, scale_ref, router_ref,
    w_buf, avg_buf, fresh, narrow, sums, scales, rbuf,
    load_sem, own_sem, sum_send, sum_recv,
    row_send, row_recv, col_send, col_recv,
    f0_send, f0_recv, f1_send, f1_recv,
    rl_sem, re_send, re_recv, rs_send, rs_recv, sc_sem,
):
    experts, rows, cols = w_ref.shape
    side = math.isqrt(shards)
    half = rows // 2
    blocks = rows // LANES
    tiles = cols // LANES
    me = lax.axis_index("shard")
    group = lax.axis_index("expert")
    r, c = me // side, me % side
    loads = min(LOADS, experts)

    def load(e):
        slot = lax.rem(e, loads)
        return (
            pltpu.make_async_copy(w_ref.at[e], w_buf.at[slot], load_sem.at[0, slot]),
            pltpu.make_async_copy(avg_ref.at[e], avg_buf.at[slot], load_sem.at[1, slot]),
        )

    for e in range(loads):
        for copy in load(e):
            copy.start()

    barrier = pltpu.get_barrier_semaphore()
    for k in range(1, shards):
        pl.semaphore_signal(barrier, inc=1, device_id={"shard": lax.rem(me + k, shards)}, device_id_type=MESH)
    for k in range(1, groups):
        pl.semaphore_signal(barrier, inc=1, device_id={"expert": lax.rem(group + k, groups)}, device_id_type=MESH)
    rbuf[...] = (rw_ref[...] * rg_ref[...]).astype(jnp.bfloat16)
    pl.semaphore_wait(barrier, shards + groups - 2)

    def remote(src, dst, send, recv, device):
        return pltpu.make_async_remote_copy(
            src_ref=src, dst_ref=dst, send_sem=send, recv_sem=recv, device_id=device, device_id_type=MESH
        )

    def sum_copy(k, e, owner):
        part = sums.at[owner, e]
        return remote(part, part, sum_send.at[k - 1, e], sum_recv.at[k - 1, e], {"shard": lax.rem(me + k, shards)})

    def place(e, h, owner):
        return out_ref.at[e, pl.ds(h * half, half), pl.ds(pl.multiple_of(owner * cols, LANES), cols)]

    def row_mate(j):
        return r * side + lax.rem(c + j, side)

    def col_mate(i):
        return lax.rem(r + i, side) * side + c

    def row_copy(j, e, h):
        return remote(
            narrow.at[e, pl.ds(h * half, half)], place(e, h, me),
            row_send.at[j - 1, 2 * e + h], row_recv.at[j - 1, 2 * e + h], {"shard": row_mate(j)},
        )

    def col_copy(i, e, h):
        return remote(
            narrow.at[e, pl.ds(h * half, half)], place(e, h, me),
            col_send.at[i - 1, 2 * e + h], col_recv.at[i - 1, 2 * e + h], {"shard": col_mate(i)},
        )

    def landed(e, h, owner, recv):
        spot = place(e, h, owner)
        remote(spot, spot, own_sem.at[0], recv, {"shard": row_mate(1)}).wait_recv()

    def f0_copy(j, i, e):
        spot = place(e, 0, row_mate(side - j))
        n = (j - 1) * (side - 1) + i - 1
        return remote(spot, spot, f0_send.at[n, e], f0_recv.at[n, e], {"shard": col_mate(i)})

    def f1_copy(j, i, e):
        spot = place(e, 1, col_mate(side - i))
        n = (j - 1) * (side - 1) + i - 1
        return remote(spot, spot, f1_send.at[n, e], f1_recv.at[n, e], {"shard": row_mate(j)})

    def far(j, i):
        return lax.rem(r + side - i, side) * side + lax.rem(c + side - j, side)

    def own_copy(e):
        return pltpu.make_async_copy(
            narrow.at[e], out_ref.at[e, :, pl.ds(pl.multiple_of(me * cols, LANES), cols)], own_sem.at[e]
        )

    def mix(e):
        slot, keep = lax.rem(e, loads), lax.rem(e, LAG + 1)
        for copy in load(e):
            copy.wait()
        share = mix_ref[e]
        rest = 1.0 - share

        @pl.loop(0, blocks)
        def _(b):
            at = pl.ds(pl.multiple_of(b * LANES, LANES), LANES)
            value = share * w_buf[slot, at, :] + rest * avg_buf[slot, at, :]
            fresh[keep, at, :] = value
            size = jnp.abs(value)
            part = size[:, :LANES]
            for t in range(1, tiles):
                part = part + size[:, t * LANES:(t + 1) * LANES]
            sums[me, e, pl.ds(b, 1), :] = jnp.sum(part.T, axis=0, keepdims=True)

        @pl.when(e + loads < experts)
        def _():
            for copy in load(e + loads):
                copy.start()

        for k in range(1, shards):
            sum_copy(k, e, me).start()

    def send(e):
        keep = lax.rem(e, LAG + 1)
        for k in range(1, shards):
            sum_copy(k, e, lax.rem(me + shards - k, shards)).wait_recv()

        @pl.loop(0, blocks)
        def _(b):
            at = pl.ds(pl.multiple_of(b * LANES, LANES), LANES)
            total = sums[0, e, pl.ds(b, 1), :]
            for s in range(1, shards):
                total = total + sums[s, e, pl.ds(b, 1), :]
            scale = total / width
            scales[e, pl.ds(b, 1), :] = scale
            inverse = jnp.broadcast_to(1.0 / scale, (LANES, LANES)).T
            for t in range(tiles):
                lane = slice(t * LANES, (t + 1) * LANES)
                narrow[e, at, lane] = (fresh[keep, at, lane] * inverse).astype(jnp.bfloat16)

        for step in range(2):
            for j in range(1, side):
                row_copy(j, e, step).start()
                col_copy(j, e, 1 - step).start()
        own_copy(e).start()

    router_own = pltpu.make_async_copy(rbuf, router_ref.at[me, group], rl_sem.at[0])

    def re_copy(k, owner):
        return remote(
            rbuf, router_ref.at[me, owner], re_send.at[k - 1], re_recv.at[k - 1],
            {"expert": lax.rem(group + k, groups)},
        )

    def rs_copy(k, owner):
        return remote(
            router_ref.at[owner], router_ref.at[owner], rs_send.at[k - 1], rs_recv.at[k - 1],
            {"shard": lax.rem(me + k, shards)},
        )

    @pl.loop(0, experts + LAG)
    def _(t):
        @pl.when(t < experts)
        def _():
            mix(t)

        @pl.when(t >= LAG)
        def _():
            send(t - LAG)

    scale_copy = pltpu.make_async_copy(scales, scale_ref, sc_sem.at[0])
    scale_copy.start()
    router_own.start()
    for k in range(1, groups):
        re_copy(k, group).start()
    router_own.wait()
    for k in range(1, groups):
        re_copy(k, lax.rem(group + groups - k, groups)).wait_recv()
    for k in range(1, shards):
        rs_copy(k, me).start()

    @pl.loop(0, experts)
    def _(e):
        for j in range(1, side):
            landed(e, 0, row_mate(side - j), row_recv.at[j - 1, 2 * e])
            for i in range(1, side):
                f0_copy(j, i, e).start()
        for i in range(1, side):
            landed(e, 1, col_mate(side - i), col_recv.at[i - 1, 2 * e + 1])
            for j in range(1, side):
                f1_copy(j, i, e).start()

    scale_copy.wait()
    for k in range(1, groups):
        re_copy(k, group).wait_send()
    for k in range(1, shards):
        rs_copy(k, me).wait_send()
        rs_copy(k, lax.rem(me + shards - k, shards)).wait_recv()

    @pl.loop(0, experts)
    def _(e):
        own_copy(e).wait()
        for k in range(1, shards):
            sum_copy(k, e, me).wait_send()
        for j in range(1, side):
            landed(e, 1, row_mate(side - j), row_recv.at[j - 1, 2 * e + 1])
            landed(e, 0, col_mate(side - j), col_recv.at[j - 1, 2 * e])
            for h in range(2):
                row_copy(j, e, h).wait_send()
                col_copy(j, e, h).wait_send()
        for j in range(1, side):
            for i in range(1, side):
                n = (j - 1) * (side - 1) + i - 1
                landed(e, 0, far(j, i), f0_recv.at[n, e])
                landed(e, 1, far(j, i), f1_recv.at[n, e])
                f0_copy(j, i, e).wait_send()
                f1_copy(j, i, e).wait_send()


def body(shards, groups, w_down, avg_down, mix_share, router_weight, router_gain):
    experts, rows, cols = w_down.shape
    side = math.isqrt(shards)
    width = shards * cols
    blocks = rows // LANES
    rw = router_weight.T
    rg = router_gain[None, :]
    dma = pltpu.SemaphoreType.DMA
    f32, bf16 = jnp.float32, jnp.bfloat16
    loads = min(LOADS, experts)
    hbm = pl.BlockSpec(memory_space=pl.ANY)
    vmem = pl.BlockSpec(memory_space=pltpu.VMEM)
    forwards = (side - 1) * (side - 1)
    serve, scale, router = pl.pallas_call(
        functools.partial(gather_kernel, shards, groups, float(width)),
        out_shape=(
            jax.ShapeDtypeStruct((experts, rows, width), bf16),
            jax.ShapeDtypeStruct((experts, blocks, LANES), f32),
            jax.ShapeDtypeStruct((shards, groups) + rw.shape, bf16),
        ),
        in_specs=[pl.BlockSpec(memory_space=pltpu.SMEM), hbm, hbm, vmem, vmem],
        out_specs=(hbm, hbm, hbm),
        scratch_shapes=[
            pltpu.VMEM((loads, rows, cols), f32),
            pltpu.VMEM((loads, rows, cols), f32),
            pltpu.VMEM((LAG + 1, rows, cols), f32),
            pltpu.VMEM((experts, rows, cols), bf16),
            pltpu.VMEM((shards, experts, blocks, LANES), f32),
            pltpu.VMEM((experts, blocks, LANES), f32),
            pltpu.VMEM(rw.shape, bf16),
            dma((2, loads)),
            dma((experts,)),
            dma((shards - 1, experts)),
            dma((shards - 1, experts)),
            dma((side - 1, 2 * experts)),
            dma((side - 1, 2 * experts)),
            dma((side - 1, 2 * experts)),
            dma((side - 1, 2 * experts)),
            dma((forwards, experts)),
            dma((forwards, experts)),
            dma((forwards, experts)),
            dma((forwards, experts)),
            dma((1,)),
            dma((groups - 1,)),
            dma((groups - 1,)),
            dma((shards - 1,)),
            dma((shards - 1,)),
            dma((1,)),
        ],
        compiler_params=pltpu.CompilerParams(collective_id=0, has_side_effects=True),
    )(mix_share, w_down, avg_down, rw, rg)
    router = router.transpose(0, 3, 1, 2).reshape(shards * rw.shape[1], groups * rw.shape[0])
    return serve, scale.reshape(experts, rows), router


def solution(mesh):
    return jax.shard_map(
        functools.partial(body, mesh.shape["shard"], mesh.shape["expert"]),
        mesh=mesh,
        in_specs=(
            P("expert", None, "shard"),
            P("expert", None, "shard"),
            P("expert"),
            P("shard", "expert"),
            P("shard"),
        ),
        out_specs=(P("expert", None, None), P("expert", None), P()),
        check_vma=False,
    )
```

```python
import functools
import math

import jax
import jax.numpy as jnp
from jax import lax
from jax.experimental import pallas as pl
from jax.experimental.pallas import tpu as pltpu
from jax.sharding import PartitionSpec as P

MESH = pl.DeviceIdType.MESH
LANES = 128
LOADS = 3
LAG = 4
CUTS = 2


def gather_kernel(
    shards, groups, width,
    mix_ref, w_ref, avg_ref, rw_ref, rg_ref,
    out_ref, scale_ref, router_ref, tail_ref,
    w_buf, avg_buf, fresh, narrow, sums, scales, rbuf,
    load_sem, own_sem, sum_send, sum_recv,
    row_send, row_recv, col_send, col_recv,
    f0_send, f0_recv, f1_send, f1_recv,
    rl_sem, re_send, re_recv, rs_send, rs_recv, sc_sem,
):
    units, rows, cols = w_ref.shape
    sent = units - 1
    side = math.isqrt(shards)
    half = rows // 2
    blocks = rows // LANES
    tiles = cols // LANES
    me = lax.axis_index("shard")
    group = lax.axis_index("expert")
    r, c = me // side, me % side
    loads = min(LOADS, units)

    def load(e):
        slot = lax.rem(e, loads)
        return (
            pltpu.make_async_copy(w_ref.at[e], w_buf.at[slot], load_sem.at[0, slot]),
            pltpu.make_async_copy(avg_ref.at[e], avg_buf.at[slot], load_sem.at[1, slot]),
        )

    for e in range(loads):
        for copy in load(e):
            copy.start()

    barrier = pltpu.get_barrier_semaphore()
    for k in range(1, shards):
        pl.semaphore_signal(barrier, inc=1, device_id={"shard": lax.rem(me + k, shards)}, device_id_type=MESH)
    for k in range(1, groups):
        pl.semaphore_signal(barrier, inc=1, device_id={"expert": lax.rem(group + k, groups)}, device_id_type=MESH)
    rbuf[...] = (rw_ref[...] * rg_ref[...]).astype(jnp.bfloat16)
    pl.semaphore_wait(barrier, shards + groups - 2)

    def remote(src, dst, send, recv, device):
        return pltpu.make_async_remote_copy(
            src_ref=src, dst_ref=dst, send_sem=send, recv_sem=recv, device_id=device, device_id_type=MESH
        )

    def sum_copy(k, e, owner):
        part = sums.at[owner, e]
        return remote(part, part, sum_send.at[k - 1, e], sum_recv.at[k - 1, e], {"shard": lax.rem(me + k, shards)})

    def place(e, h, owner):
        return out_ref.at[e, pl.ds(h * half, half), pl.ds(pl.multiple_of(owner * cols, LANES), cols)]

    def row_mate(j):
        return r * side + lax.rem(c + j, side)

    def col_mate(i):
        return lax.rem(r + i, side) * side + c

    def whole(e, owner):
        return out_ref.at[e, :, pl.ds(pl.multiple_of(owner * cols, LANES), cols)]

    def row_copy(j, e):
        return remote(
            narrow.at[e], whole(e, me), row_send.at[j - 1, e], row_recv.at[j - 1, e], {"shard": row_mate(j)}
        )

    def col_copy(i, e):
        return remote(
            narrow.at[e], whole(e, me), col_send.at[i - 1, e], col_recv.at[i - 1, e], {"shard": col_mate(i)}
        )

    def landed(spot, recv):
        remote(spot, spot, own_sem.at[0], recv, {"shard": row_mate(1)}).wait_recv()

    def f0_copy(j, i, e):
        spot = place(e, 0, row_mate(side - j))
        n = (j - 1) * (side - 1) + i - 1
        return remote(spot, spot, f0_send.at[n, e], f0_recv.at[n, e], {"shard": col_mate(i)})

    def f1_copy(j, i, e):
        spot = place(e, 1, col_mate(side - i))
        n = (j - 1) * (side - 1) + i - 1
        return remote(spot, spot, f1_send.at[n, e], f1_recv.at[n, e], {"shard": row_mate(j)})

    def far(j, i):
        return lax.rem(r + side - i, side) * side + lax.rem(c + side - j, side)

    def own_copy(e):
        return pltpu.make_async_copy(narrow.at[e], whole(e, me), own_sem.at[e])

    tail_copy = pltpu.make_async_copy(narrow.at[sent], tail_ref, own_sem.at[sent])

    def mix(e):
        slot, keep = lax.rem(e, loads), lax.rem(e, LAG + 1)
        for copy in load(e):
            copy.wait()
        share = mix_ref[e // CUTS]
        rest = 1.0 - share

        @pl.loop(0, blocks)
        def _(b):
            at = pl.ds(pl.multiple_of(b * LANES, LANES), LANES)
            value = share * w_buf[slot, at, :] + rest * avg_buf[slot, at, :]
            fresh[keep, at, :] = value
            size = jnp.abs(value)
            part = size[:, :LANES]
            for t in range(1, tiles):
                part = part + size[:, t * LANES:(t + 1) * LANES]
            sums[me, e, pl.ds(b, 1), :] = jnp.sum(part.T, axis=0, keepdims=True)

        @pl.when(e + loads < units)
        def _():
            for copy in load(e + loads):
                copy.start()

        for k in range(1, shards):
            sum_copy(k, e, me).start()

    def send(e):
        keep = lax.rem(e, LAG + 1)
        for k in range(1, shards):
            sum_copy(k, e, lax.rem(me + shards - k, shards)).wait_recv()

        @pl.loop(0, blocks)
        def _(b):
            at = pl.ds(pl.multiple_of(b * LANES, LANES), LANES)
            total = sums[0, e, pl.ds(b, 1), :]
            for s in range(1, shards):
                total = total + sums[s, e, pl.ds(b, 1), :]
            scale = total / width
            scales[e, pl.ds(b, 1), :] = scale
            inverse = jnp.broadcast_to(1.0 / scale, (LANES, LANES)).T
            for t in range(tiles):
                lane = slice(t * LANES, (t + 1) * LANES)
                narrow[e, at, lane] = (fresh[keep, at, lane] * inverse).astype(jnp.bfloat16)

        @pl.when(e < sent)
        def _():
            for j in range(1, side):
                row_copy(j, e).start()
                col_copy(j, e).start()
            own_copy(e).start()

    router_own = pltpu.make_async_copy(rbuf, router_ref.at[me, group], rl_sem.at[0])

    def re_copy(k, owner):
        return remote(
            rbuf, router_ref.at[me, owner], re_send.at[k - 1], re_recv.at[k - 1],
            {"expert": lax.rem(group + k, groups)},
        )

    def rs_copy(k, owner):
        return remote(
            router_ref.at[owner], router_ref.at[owner], rs_send.at[k - 1], rs_recv.at[k - 1],
            {"shard": lax.rem(me + k, shards)},
        )

    @pl.loop(0, units + LAG)
    def _(t):
        @pl.when(t < units)
        def _():
            mix(t)

        @pl.when(t >= LAG)
        def _():
            send(t - LAG)

    scale_copy = pltpu.make_async_copy(scales, scale_ref, sc_sem.at[0])
    scale_copy.start()
    tail_copy.start()
    router_own.start()
    for k in range(1, groups):
        re_copy(k, group).start()
    router_own.wait()
    for k in range(1, groups):
        re_copy(k, lax.rem(group + groups - k, groups)).wait_recv()
    for k in range(1, shards):
        rs_copy(k, me).start()

    @pl.loop(0, sent)
    def _(e):
        for j in range(1, side):
            landed(whole(e, row_mate(side - j)), row_recv.at[j - 1, e])
            for i in range(1, side):
                f0_copy(j, i, e).start()
        for i in range(1, side):
            landed(whole(e, col_mate(side - i)), col_recv.at[i - 1, e])
            for j in range(1, side):
                f1_copy(j, i, e).start()

    scale_copy.wait()
    tail_copy.wait()
    for k in range(1, groups):
        re_copy(k, group).wait_send()
    for k in range(1, shards):
        rs_copy(k, me).wait_send()
        rs_copy(k, lax.rem(me + shards - k, shards)).wait_recv()

    @pl.loop(0, units)
    def _(e):
        for k in range(1, shards):
            sum_copy(k, e, me).wait_send()

    @pl.loop(0, sent)
    def _(e):
        own_copy(e).wait()
        for j in range(1, side):
            row_copy(j, e).wait_send()
            col_copy(j, e).wait_send()
        for j in range(1, side):
            for i in range(1, side):
                n = (j - 1) * (side - 1) + i - 1
                landed(place(e, 0, far(j, i)), f0_recv.at[n, e])
                landed(place(e, 1, far(j, i)), f1_recv.at[n, e])
                f0_copy(j, i, e).wait_send()
                f1_copy(j, i, e).wait_send()


def copy_kernel(from_ref, to_ref):
    to_ref[...] = from_ref[...]


def place_kernel(shards, *refs):
    pieces, out_ref, sem = refs[:shards], refs[shards + 1], refs[shards + 2]
    me = lax.axis_index("shard")
    cols = pieces[0].shape[1]
    last = out_ref.shape[0] - 1
    copies = []
    for k in range(shards):
        owner = lax.rem(me + shards - k, shards)
        spot = out_ref.at[last, :, pl.ds(pl.multiple_of(owner * cols, LANES), cols)]
        copies.append(pltpu.make_async_copy(pieces[k], spot, sem.at[k]))
    for copy in copies:
        copy.start()
    for copy in copies:
        copy.wait()


def body(shards, groups, w_down, avg_down, mix_share, router_weight, router_gain):
    experts, full, cols = w_down.shape
    units, rows = experts * CUTS, full // CUTS
    sent = units - 1
    side = math.isqrt(shards)
    width = shards * cols
    blocks = rows // LANES
    rw = router_weight.T
    rg = router_gain[None, :]
    dma = pltpu.SemaphoreType.DMA
    f32, bf16 = jnp.float32, jnp.bfloat16
    loads = min(LOADS, units)
    hbm = pl.BlockSpec(memory_space=pl.ANY)
    vmem = pl.BlockSpec(memory_space=pltpu.VMEM)
    forwards = (side - 1) * (side - 1)
    parts, scale, router, tail = pl.pallas_call(
        functools.partial(gather_kernel, shards, groups, float(width)),
        out_shape=(
            jax.ShapeDtypeStruct((sent, rows, width), bf16),
            jax.ShapeDtypeStruct((units, blocks, LANES), f32),
            jax.ShapeDtypeStruct((shards, groups) + rw.shape, bf16),
            jax.ShapeDtypeStruct((rows, cols), bf16),
        ),
        in_specs=[pl.BlockSpec(memory_space=pltpu.SMEM), hbm, hbm, vmem, vmem],
        out_specs=(hbm, hbm, hbm, hbm),
        scratch_shapes=[
            pltpu.VMEM((loads, rows, cols), f32),
            pltpu.VMEM((loads, rows, cols), f32),
            pltpu.VMEM((LAG + 1, rows, cols), f32),
            pltpu.VMEM((units, rows, cols), bf16),
            pltpu.VMEM((shards, units, blocks, LANES), f32),
            pltpu.VMEM((units, blocks, LANES), f32),
            pltpu.VMEM(rw.shape, bf16),
            dma((2, loads)),
            dma((units,)),
            dma((shards - 1, units)),
            dma((shards - 1, units)),
            dma((side - 1, sent)),
            dma((side - 1, sent)),
            dma((side - 1, sent)),
            dma((side - 1, sent)),
            dma((forwards, sent)),
            dma((forwards, sent)),
            dma((forwards, sent)),
            dma((forwards, sent)),
            dma((1,)),
            dma((groups - 1,)),
            dma((groups - 1,)),
            dma((shards - 1,)),
            dma((shards - 1,)),
            dma((1,)),
        ],
        compiler_params=pltpu.CompilerParams(collective_id=0, has_side_effects=True),
    )(mix_share, w_down.reshape(units, rows, cols), avg_down.reshape(units, rows, cols), rw, rg)
    pieces = [tail]
    for k in range(1, shards):
        pieces.append(lax.ppermute(tail, "shard", [(s, (s + k) % shards) for s in range(shards)]))
    block = pl.BlockSpec((1, rows, width), lambda i: (i, 0, 0))
    whole = jax.ShapeDtypeStruct((units, rows, width), bf16)
    held = pl.pallas_call(
        copy_kernel,
        grid=(sent,),
        out_shape=whole,
        in_specs=[block],
        out_specs=block,
        cost_estimate=pl.CostEstimate(flops=0, bytes_accessed=4 * sent * rows * width, transcendentals=0),
    )(parts)
    serve = pl.pallas_call(
        functools.partial(place_kernel, shards),
        out_shape=whole,
        in_specs=[hbm] * shards + [hbm],
        out_specs=hbm,
        input_output_aliases={shards: 0},
        scratch_shapes=[dma((shards,))],
        compiler_params=pltpu.CompilerParams(vmem_limit_bytes=8 * 2 ** 20),
    )(*pieces, held)
    router = router.transpose(0, 3, 1, 2).reshape(shards * rw.shape[1], groups * rw.shape[0])
    return serve.reshape(experts, full, width), scale.reshape(experts, full), router


def solution(mesh):
    return jax.shard_map(
        functools.partial(body, mesh.shape["shard"], mesh.shape["expert"]),
        mesh=mesh,
        in_specs=(
            P("expert", None, "shard"),
            P("expert", None, "shard"),
            P("expert"),
            P("shard", "expert"),
            P("shard"),
        ),
        out_specs=(P("expert", None, None), P("expert", None), P()),
        check_vma=False,
    )
```
